256 devices in a mesh: gx: 8 (over y, core), gz: 8 (over z), gy: 4 (over x).
Axes of the slice: x: 4, y: 4, z: 8, core: 2. Of those that a mesh axis runs over, the one named last changes fastest.
Arguments:
- logits: float32 [256, 1048576], P('gy', ('gx', 'gz')), may hold values from -60 to 250
Outputs:
- token_potential: float32 [1048576], P(('gx', 'gz'))
- expert_potential: float32 [256], P('gy')
The draws below stay inside these ranges and needn't reach their ends.
All inputs are finite; a program needn't handle non-finite values.
Results may differ from the reference program's by a relative error of at most 0.0001.
Values sent between devices are 32-bit elements; how exact they have to be, the bound alone decides.
No kernel may reach another device: no remote copies, remote signals or barrier semaphores. Data moves between devices by JAX's collectives and lax.ppermute only.
A program may use at most 64 MiB of HBM per device.

```python
import jax
import jax.numpy as jnp

E = 256
ITERS = 3
TOKENS = 1048576


def draw_logits(key, part):
    keys = jax.random.split(jax.random.fold_in(key, 11), 2)
    place = jnp.arange(TOKENS, dtype=jnp.float32) / jnp.float32(TOKENS)
    spread = (3.0 + 3.0 * place)[None, :]
    offset = jax.random.uniform(keys[1], (E, 1), jnp.float32, -1.5, 1.5)
    values = jax.random.normal(keys[0], (E, TOKENS), jnp.float32) * spread + offset
    token_ids = jnp.arange(TOKENS, dtype=jnp.int32)[None, :]
    row_ids = jnp.arange(E, dtype=jnp.int32)[:, None]
    lowest = (token_ids % 4096 == 3) & (row_ids == token_ids * 7 % E)
    values = jnp.where(lowest, -60.0, values)
    return jnp.clip(values, -60.0, 250.0).astype(jnp.float32)


def setup_inputs(seed: int = 0) -> dict:
    streams_of = jax.random.split(jax.random.key(seed), 2)
    logits = draw_logits(jax.random.fold_in(streams_of[1], 71), 0)
    return {"logits": logits}


def reference(logits):
    log_cap = jnp.log(jnp.float32(TOKENS) / jnp.float32(E))
    token_potential = jnp.zeros((TOKENS,), jnp.float32)
    expert_potential = jnp.zeros((E,), jnp.float32)
    for step in range(ITERS):
        shifted = logits + token_potential[None, :]
        top = jnp.max(shifted, axis=1)
        total = jnp.sum(jnp.exp(shifted - top[:, None]), axis=1)
        expert_potential = log_cap - (top + jnp.log(total))
        raised = logits + expert_potential[:, None]
        peak = jnp.max(raised, axis=0)
        summed = jnp.sum(jnp.exp(raised - peak[None, :]), axis=0)
        token_potential = -(peak + jnp.log(summed))
    return token_potential, expert_potential
```

```python
import functools

import numpy as np

import jax
import jax.numpy as jnp
from jax import lax
from jax.experimental import pallas as pl
from jax.experimental.pallas import tpu as pltpu
from jax.sharding import PartitionSpec as P

ITERS = 3
LANES = 128
CHUNKS = 8
UNROLL = 8
VMEM = pl.BlockSpec(memory_space=pltpu.VMEM)
HBM = pl.BlockSpec(memory_space=pltpu.HBM)


def lane_block(j):
    return pl.ds(pl.multiple_of(j * LANES, LANES), LANES)


def rows_to_lanes(values, experts):
    below = jnp.zeros((LANES - experts, LANES), jnp.float32)
    square = jnp.concatenate([values, below], axis=0)
    return jnp.sum(square.T, axis=0, keepdims=True)


def lanes_to_rows(row, experts):
    return jnp.broadcast_to(row, (LANES, LANES)).T[:experts]


def row_lse_kernel(x_hbm, x_ref, msg_ref, sems):
    experts, tokens = x_ref.shape
    width = tokens // CHUNKS
    copies = [
        pltpu.make_async_copy(
            x_hbm.at[:, pl.ds(i * width, width)],
            x_ref.at[:, pl.ds(i * width, width)],
            sems.at[i],
        )
        for i in range(CHUNKS)
    ]
    for copy in copies:
        copy.start()
    top = jnp.full((experts, LANES), -jnp.inf, jnp.float32)
    total = jnp.zeros((experts, LANES), jnp.float32)
    for i, copy in enumerate(copies):
        copy.wait()
        starts = range(i * width, (i + 1) * width, LANES)
        new = top
        for s in starts:
            new = jnp.maximum(new, x_ref[:, pl.ds(s, LANES)])
        if i:
            total = total * jnp.exp(top - new)
        top = new
        for s in starts:
            total = total + jnp.exp(x_ref[:, pl.ds(s, LANES)] - top)
    peak = jnp.max(top, axis=1, keepdims=True)
    summed = jnp.sum(total * jnp.exp(top - peak), axis=1, keepdims=True)
    lse = peak + jnp.log(summed)
    below = jnp.zeros((LANES - experts, LANES), jnp.float32)
    square = jnp.concatenate([jnp.broadcast_to(lse, (experts, LANES)), below], axis=0)
    msg_ref[...] = jnp.broadcast_to(square.T[:1][None], msg_ref.shape)


def column_lse_kernel(log_cap, got_ref, x_ref, e_ref, peak_ref, msg_ref, ep_ref, sum_ref):
    experts, tokens = x_ref.shape
    parts = got_ref[...]
    top = jnp.max(parts, axis=0)
    ep = log_cap - (top + jnp.log(jnp.sum(jnp.exp(parts - top[None]), axis=0)))
    ep_ref[...] = ep
    shift = lanes_to_rows(ep, experts)

    def step(k, carry):
        for n in range(UNROLL):
            j = k * UNROLL + n
            raised = x_ref[:, lane_block(j)] + shift
            peak = jnp.max(raised, axis=0, keepdims=True)
            e = jnp.exp(raised - peak)
            e_ref[:, lane_block(j)] = e
            peak_ref[pl.ds(j, 1), :] = peak
            sum_ref[pl.ds(j, 1), :] = jnp.sum(e, axis=0, keepdims=True)
        return carry

    lax.fori_loop(0, tokens // (LANES * UNROLL), step, 0)
    msg_ref[...] = jnp.broadcast_to((peak_ref[...] + jnp.log(sum_ref[...]))[None], msg_ref.shape)


def weighted_rows(e_ref, w_ref, msg_ref):
    experts, tokens = e_ref.shape

    def step(k, acc):
        for n in range(UNROLL):
            j = k * UNROLL + n
            acc = acc + e_ref[:, lane_block(j)] * w_ref[pl.ds(j, 1), :]
        return acc

    zero = jnp.zeros((experts, LANES), jnp.float32)
    acc = lax.fori_loop(0, tokens // (LANES * UNROLL), step, zero)
    msg_ref[...] = jnp.broadcast_to(rows_to_lanes(acc, experts)[None], msg_ref.shape)


def first_rows_kernel(got_ref, peak_ref, e_ref, msg_ref, f_ref, tp_ref):
    parts = got_ref[...]
    top = jnp.max(parts, axis=0)
    tp = -(top + jnp.log(jnp.sum(jnp.exp(parts - top[None]), axis=0)))
    tp_ref[...] = tp
    f_ref[...] = jnp.exp(peak_ref[...] + tp)
    weighted_rows(e_ref, f_ref, msg_ref)


def rows_kernel(got_ref, f_ref, e_ref, msg_ref, w_ref):
    w_ref[...] = f_ref[...] / jnp.sum(got_ref[...], axis=0)
    weighted_rows(e_ref, w_ref, msg_ref)


def columns_kernel(cap, log_cap, got_ref, ep1_ref, f_ref, e_ref, msg_ref, ep_ref, sum_ref):
    experts, tokens = e_ref.shape
    r = jnp.sum(got_ref[...], axis=0)
    r = jnp.where(lax.broadcasted_iota(jnp.int32, r.shape, 1) < experts, r, 1.0)
    ep_ref[...] = (ep1_ref[...] + (log_cap - jnp.log(r)))[:, :experts]
    u = lanes_to_rows(cap / r, experts)

    def step(k, carry):
        for n in range(UNROLL):
            j = k * UNROLL + n
            sum_ref[pl.ds(j, 1), :] = jnp.sum(e_ref[:, lane_block(j)] * u, axis=0, keepdims=True)
        return carry

    lax.fori_loop(0, tokens // (LANES * UNROLL), step, 0)
    msg_ref[...] = jnp.broadcast_to((f_ref[...] * sum_ref[...])[None], msg_ref.shape)


def last_kernel(got_ref, tp1_ref, tp_ref):
    tp_ref[...] = tp1_ref[...] - jnp.log(jnp.sum(got_ref[...], axis=0))


def call(kernel, shapes, args, scratch=(), specs=None, limit=24):
    return pl.pallas_call(
        kernel,
        out_shape=[jax.ShapeDtypeStruct(s, jnp.float32) for s in shapes],
        in_specs=specs or [VMEM] * len(args),
        out_specs=[VMEM] * len(shapes),
        scratch_shapes=list(scratch),
        compiler_params=pltpu.CompilerParams(vmem_limit_bytes=limit * 1024 * 1024),
    )(*args)


def exchange(array, axis):
    return lax.all_to_all(array, axis, split_axis=0, concat_axis=0, tiled=True)


def per_device(logits):
    experts, tokens = logits.shape
    token_axes, expert_axis = ("gx", "gz"), "gy"
    token_shards, expert_shards = lax.axis_size(token_axes), lax.axis_size(expert_axis)
    cap = float(tokens * token_shards) / float(experts * expert_shards)
    log_cap = float(np.log(np.float32(cap)))
    rows = tokens // LANES
    big, flat, one = (experts, tokens), (rows, LANES), (1, LANES)
    to_rows = (token_shards, 1, LANES)
    to_cols = (expert_shards, rows, LANES)
    flat_scratch = pltpu.VMEM(flat, jnp.float32)

    x, msg = call(
        row_lse_kernel, [big, to_rows], [logits],
        [pltpu.SemaphoreType.DMA((CHUNKS,))], [HBM], 49,
    )
    got = exchange(msg, token_axes)
    e, peak, msg, ep1 = call(
        functools.partial(column_lse_kernel, log_cap),
        [big, flat, to_cols, one], [got, x], [flat_scratch],
    )
    got = exchange(msg, expert_axis)
    msg, f, tp1 = call(first_rows_kernel, [to_rows, flat, flat], [got, peak, e])
    for step in range(1, ITERS):
        got = exchange(msg, token_axes)
        msg, ep = call(
            functools.partial(columns_kernel, cap, log_cap),
            [to_cols, (1, experts)], [got, ep1, f, e], [flat_scratch],
        )
        got = exchange(msg, expert_axis)
        if step < ITERS - 1:
            (msg,) = call(rows_kernel, [to_rows], [got, f, e], [flat_scratch])
    (tp,) = call(last_kernel, [flat], [got, tp1])
    return tp.reshape(tokens), ep.reshape(experts)


def solution(mesh):
    in_specs = (P("gy", ("gx", "gz")),)
    out_specs = (P(("gx", "gz")), P("gy"))
    return jax.shard_map(
        per_device, mesh=mesh, in_specs=in_specs, out_specs=out_specs, check_vma=False
    )
```

```python
import functools

import numpy as np

import jax
import jax.numpy as jnp
from jax import lax
from jax.experimental import pallas as pl
from jax.experimental.pallas import tpu as pltpu
from jax.sharding import PartitionSpec as P

ITERS = 3
LANES = 128
SUB = 8
CHUNKS = 8
UNROLL = 8
VMEM = pl.BlockSpec(memory_space=pltpu.VMEM)
HBM = pl.BlockSpec(memory_space=pltpu.HBM)


def tile(ref, j):
    block = ref[:, pl.ds(pl.multiple_of(j * LANES, LANES), LANES)]
    return block.reshape(-1, SUB, LANES)


def classes(j):
    return pl.ds(pl.multiple_of(j * SUB, SUB), SUB)


def class_rows(ref, block, s):
    return ref[pl.ds(block * SUB * SUB + s, SUB, stride=SUB), :]


def rows_to_lanes(values):
    return jnp.sum(values.T, axis=0, keepdims=True)


def lanes_to_rows(row):
    square = jnp.broadcast_to(row, (LANES, row.shape[1])).T
    return square.reshape(-1, SUB, LANES)


def for_tiles(count, body, carry):
    def step(k, carry):
        for n in range(UNROLL):
            carry = body(k * UNROLL + n, carry)
        return carry

    return lax.fori_loop(0, count // UNROLL, step, carry)


def row_lse_kernel(x_hbm, x_ref, msg_ref, sems):
    experts, tokens = x_ref.shape
    width = tokens // CHUNKS
    copies = [
        pltpu.make_async_copy(
            x_hbm.at[:, pl.ds(i * width, width)],
            x_ref.at[:, pl.ds(i * width, width)],
            sems.at[i],
        )
        for i in range(CHUNKS)
    ]
    for copy in copies:
        copy.start()
    top = jnp.full((experts, LANES), -jnp.inf, jnp.float32)
    total = jnp.zeros((experts, LANES), jnp.float32)
    for i, copy in enumerate(copies):
        copy.wait()
        starts = range(i * width, (i + 1) * width, LANES)
        new = top
        for s in starts:
            new = jnp.maximum(new, x_ref[:, pl.ds(s, LANES)])
        if i:
            total = total * jnp.exp(top - new)
        top = new
        for s in starts:
            total = total + jnp.exp(x_ref[:, pl.ds(s, LANES)] - top)
    tops, totals = top.T, total.T
    peak = jnp.max(tops, axis=0, keepdims=True)
    summed = jnp.sum(totals * jnp.exp(tops - peak), axis=0, keepdims=True)
    msg_ref[...] = jnp.broadcast_to((peak + jnp.log(summed))[None], msg_ref.shape)


def column_lse_kernel(log_cap, got_ref, x_ref, e_ref, top_ref, msg_ref, ep_ref, sum_ref):
    tokens = x_ref.shape[1]
    parts = got_ref[...]
    most = jnp.max(parts, axis=0)
    ep = log_cap - (most + jnp.log(jnp.sum(jnp.exp(parts - most[None]), axis=0)))
    ep_ref[...] = ep
    shift = lanes_to_rows(ep)

    def body(j, carry):
        raised = tile(x_ref, j) + shift
        top = jnp.max(raised, axis=0)
        e = jnp.exp(raised - top[None])
        e_ref[:, pl.ds(pl.multiple_of(j * LANES, LANES), LANES)] = e.reshape(-1, LANES)
        top_ref[classes(j), :] = top
        sum_ref[classes(j), :] = jnp.sum(e, axis=0)
        return carry

    for_tiles(tokens // LANES, body, 0)
    for b in range(tokens // (LANES * SUB)):
        tops = [class_rows(top_ref, b, s) for s in range(SUB)]
        peak = functools.reduce(jnp.maximum, tops)
        total = sum(
            class_rows(sum_ref, b, s) * jnp.exp(tops[s] - peak) for s in range(SUB)
        )
        msg_ref[classes(b), :] = peak + jnp.log(total)


def joined(one, two, three, four):
    return (one + two) + (three + four)


def first_rows_kernel(own, g1, g2, g3, top_ref, e_ref, msg_ref, f_ref, tp_ref):
    experts, tokens = e_ref.shape
    parts = [ref[...] for ref in (own, g1, g2, g3)]
    peak = functools.reduce(jnp.maximum, parts)
    tp_ref[...] = -(peak + jnp.log(joined(*(jnp.exp(part - peak) for part in parts))))

    def body(j, acc):
        f = jnp.exp(top_ref[classes(j), :] + tp_ref[pl.ds(j, 1), :])
        f_ref[classes(j), :] = f
        return acc + tile(e_ref, j) * f[None]

    zero = jnp.zeros((experts // SUB, SUB, LANES), jnp.float32)
    acc = for_tiles(tokens // LANES, body, zero)
    msg_ref[...] = jnp.broadcast_to(
        rows_to_lanes(acc.reshape(experts, LANES))[None], msg_ref.shape
    )


def rows_kernel(own, g1, g2, g3, f_ref, e_ref, msg_ref, v_ref):
    experts, tokens = e_ref.shape
    v_ref[...] = 1.0 / joined(own[...], g1[...], g2[...], g3[...])

    def body(j, acc):
        w = f_ref[classes(j), :] * v_ref[pl.ds(j, 1), :]
        return acc + tile(e_ref, j) * w[None]

    zero = jnp.zeros((experts // SUB, SUB, LANES), jnp.float32)
    acc = for_tiles(tokens // LANES, body, zero)
    msg_ref[...] = jnp.broadcast_to(
        rows_to_lanes(acc.reshape(experts, LANES))[None], msg_ref.shape
    )


def columns_kernel(cap, got_ref, f_ref, e_ref, msg_ref, sum_ref):
    tokens = e_ref.shape[1]
    u = lanes_to_rows(cap / jnp.sum(got_ref[...], axis=0))

    def body(j, carry):
        sum_ref[classes(j), :] = jnp.sum(tile(e_ref, j) * u, axis=0) * f_ref[classes(j), :]
        return carry

    for_tiles(tokens // LANES, body, 0)
    for b in range(tokens // (LANES * SUB)):
        msg_ref[classes(b), :] = sum(class_rows(sum_ref, b, s) for s in range(SUB))


def last_kernel(log_cap, own, g1, g2, g3, tp1_ref, got_ref, ep1_ref, tp_ref, ep_ref):
    ep_ref[...] = ep1_ref[...] + (log_cap - jnp.log(jnp.sum(got_ref[...], axis=0)))
    tp_ref[...] = tp1_ref[...] - jnp.log(joined(own[...], g1[...], g2[...], g3[...]))


def call(kernel, shapes, args, scratch=(), specs=None, limit=24):
    return pl.pallas_call(
        kernel,
        out_shape=[jax.ShapeDtypeStruct(s, jnp.float32) for s in shapes],
        in_specs=specs or [VMEM] * len(args),
        out_specs=[VMEM] * len(shapes),
        scratch_shapes=list(scratch),
        compiler_params=pltpu.CompilerParams(vmem_limit_bytes=limit * 1024 * 1024),
    )(*args)


def over_tokens(array, axes):
    return lax.all_to_all(array, axes, split_axis=0, concat_axis=0, tiled=True)


def over_experts(array, axis):
    members = range(lax.axis_size(axis))
    return [array] + [
        lax.ppermute(array, axis, [(i, i ^ s) for i in members]) for s in members if s
    ]


def per_device(logits):
    experts, tokens = logits.shape
    token_axes, expert_axis = ("gx", "gz"), "gy"
    token_shards, expert_shards = lax.axis_size(token_axes), lax.axis_size(expert_axis)
    cap = float(tokens * token_shards) / float(experts * expert_shards)
    log_cap = float(np.log(np.float32(cap)))
    rows = tokens // LANES
    big, flat, wide, one = (experts, tokens), (rows, LANES), (rows * SUB, LANES), (1, experts)
    to_rows = (token_shards, 1, experts)

    x, msg = call(
        row_lse_kernel, [big, to_rows], [logits],
        [pltpu.SemaphoreType.DMA((CHUNKS,))], [HBM], 49,
    )
    got = over_tokens(msg, token_axes)
    e, top, msg, ep1 = call(
        functools.partial(column_lse_kernel, log_cap),
        [big, wide, flat, one], [got, x], [pltpu.VMEM(wide, jnp.float32)],
    )
    got = over_experts(msg, expert_axis)
    msg, f, tp1 = call(first_rows_kernel, [to_rows, wide, flat], [*got, top, e])
    for step in range(1, ITERS):
        row_parts = over_tokens(msg, token_axes)
        (msg,) = call(
            functools.partial(columns_kernel, cap),
            [flat], [row_parts, f, e], [pltpu.VMEM(wide, jnp.float32)],
        )
        got = over_experts(msg, expert_axis)
        if step < ITERS - 1:
            (msg,) = call(
                rows_kernel, [to_rows], [*got, f, e], [pltpu.VMEM(flat, jnp.float32)]
            )
    tp, ep = call(
        functools.partial(last_kernel, log_cap),
        [flat, one], [*got, tp1, row_parts, ep1],
    )
    return tp.reshape(tokens), ep.reshape(experts)


def solution(mesh):
    in_specs = (P("gy", ("gx", "gz")),)
    out_specs = (P(("gx", "gz")), P("gy"))
    return jax.shard_map(
        per_device, mesh=mesh, in_specs=in_specs, out_specs=out_specs, check_vma=False
    )
```

```python
import functools

import numpy as np

import jax
import jax.numpy as jnp
from jax import lax
from jax.experimental import pallas as pl
from jax.experimental.pallas import tpu as pltpu
from jax.sharding import PartitionSpec as P

ITERS = 3
LANES = 128
SUB = 8
UNROLL = 128
VMEM = pl.BlockSpec(memory_space=pltpu.VMEM)
HBM = pl.BlockSpec(memory_space=pltpu.HBM)


def tile(ref, j):
    block = ref[:, pl.ds(pl.multiple_of(j * LANES, LANES), LANES)]
    return block.reshape(-1, SUB, LANES)


def classes(j):
    return pl.ds(pl.multiple_of(j * SUB, SUB), SUB)


def class_rows(ref, block, s):
    return ref[pl.ds(block * SUB * SUB + s, SUB, stride=SUB), :]


def rows_to_lanes(values):
    return jnp.sum(values.T, axis=0, keepdims=True)


def lanes_to_rows(row):
    square = jnp.broadcast_to(row, (LANES, row.shape[1])).T
    return square.reshape(-1, SUB, LANES)


def for_tiles(count, body, carry):
    def step(k, carry):
        for n in range(UNROLL):
            carry = body(k * UNROLL + n, carry)
        return carry

    return lax.fori_loop(0, count // UNROLL, step, carry)


def row_lse_kernel(x_hbm, x_ref, msg_ref, sems):
    experts, tokens = x_ref.shape
    blocks = [pl.ds(g * SUB, SUB) for g in range(experts // SUB)]
    copies = [
        pltpu.make_async_copy(x_hbm.at[block, :], x_ref.at[block, :], sems.at[g])
        for g, block in enumerate(blocks)
    ]
    for copy in copies:
        copy.start()
    tops, totals = [], []
    for copy, block in zip(copies, blocks):
        copy.wait()
        starts = range(0, tokens, LANES)
        tree = [x_ref[block, pl.ds(s, LANES)] for s in starts]
        while len(tree) > 1:
            tree = [jnp.maximum(*pair) for pair in zip(tree[::2], tree[1::2])]
        top = tree[0]
        parts = [jnp.zeros((SUB, LANES), jnp.float32)] * 4
        for n, s in enumerate(starts):
            parts[n % 4] = parts[n % 4] + jnp.exp(x_ref[block, pl.ds(s, LANES)] - top)
        tops.append(top)
        totals.append((parts[0] + parts[1]) + (parts[2] + parts[3]))
    tops, totals = jnp.concatenate(tops).T, jnp.concatenate(totals).T
    peak = jnp.max(tops, axis=0, keepdims=True)
    summed = jnp.sum(totals * jnp.exp(tops - peak), axis=0, keepdims=True)
    msg_ref[...] = jnp.broadcast_to((peak + jnp.log(summed))[None], msg_ref.shape)


def column_lse_kernel(log_cap, got_ref, x_ref, e_ref, top_ref, msg_ref, ep_ref, sum_ref):
    tokens = x_ref.shape[1]
    parts = got_ref[...]
    most = jnp.max(parts, axis=0)
    ep = log_cap - (most + jnp.log(jnp.sum(jnp.exp(parts - most[None]), axis=0)))
    ep_ref[...] = ep
    shift = lanes_to_rows(ep)

    def body(j, carry):
        raised = tile(x_ref, j) + shift
        top = jnp.max(raised, axis=0)
        e = jnp.exp(raised - top[None])
        e_ref[:, pl.ds(pl.multiple_of(j * LANES, LANES), LANES)] = e.reshape(-1, LANES)
        top_ref[classes(j), :] = top
        sum_ref[classes(j), :] = jnp.sum(e, axis=0)
        return carry

    for_tiles(tokens // LANES, body, 0)
    for b in range(tokens // (LANES * SUB)):
        tops = [class_rows(top_ref, b, s) for s in range(SUB)]
        peak = functools.reduce(jnp.maximum, tops)
        total = sum(
            class_rows(sum_ref, b, s) * jnp.exp(tops[s] - peak) for s in range(SUB)
        )
        msg_ref[classes(b), :] = peak + jnp.log(total)


def joined(one, two, three, four):
    return (one + two) + (three + four)


def first_rows_kernel(own, g1, g2, g3, top_ref, e_ref, msg_ref, f_ref, tp_ref):
    experts, tokens = e_ref.shape
    parts = [ref[...] for ref in (own, g1, g2, g3)]
    peak = functools.reduce(jnp.maximum, parts)
    tp_ref[...] = -(peak + jnp.log(joined(*(jnp.exp(part - peak) for part in parts))))

    def body(j, acc):
        f = jnp.exp(top_ref[classes(j), :] + tp_ref[pl.ds(j, 1), :])
        f_ref[classes(j), :] = f
        return acc[1], acc[0] + tile(e_ref, j) * f[None]

    zero = jnp.zeros((experts // SUB, SUB, LANES), jnp.float32)
    acc = sum(for_tiles(tokens // LANES, body, (zero, zero)))
    msg_ref[...] = jnp.broadcast_to(
        rows_to_lanes(acc.reshape(experts, LANES))[None], msg_ref.shape
    )


def rows_kernel(own, g1, g2, g3, f_ref, e_ref, msg_ref, v_ref):
    experts, tokens = e_ref.shape
    v_ref[...] = 1.0 / joined(own[...], g1[...], g2[...], g3[...])

    def body(j, acc):
        w = f_ref[classes(j), :] * v_ref[pl.ds(j, 1), :]
        return acc[1], acc[0] + tile(e_ref, j) * w[None]

    zero = jnp.zeros((experts // SUB, SUB, LANES), jnp.float32)
    acc = sum(for_tiles(tokens // LANES, body, (zero, zero)))
    msg_ref[...] = jnp.broadcast_to(
        rows_to_lanes(acc.reshape(experts, LANES))[None], msg_ref.shape
    )


def columns_kernel(cap, got_ref, f_ref, e_ref, msg_ref, sum_ref):
    tokens = e_ref.shape[1]
    u = lanes_to_rows(cap / jnp.sum(got_ref[...], axis=0))

    def body(j, carry):
        sum_ref[classes(j), :] = jnp.sum(tile(e_ref, j) * u, axis=0) * f_ref[classes(j), :]
        return carry

    for_tiles(tokens // LANES, body, 0)
    for b in range(tokens // (LANES * SUB)):
        msg_ref[classes(b), :] = sum(class_rows(sum_ref, b, s) for s in range(SUB))


def last_kernel(log_cap, own, g1, g2, g3, tp1_ref, got_ref, ep1_ref, tp_ref, ep_ref):
    ep_ref[...] = ep1_ref[...] + (log_cap - jnp.log(jnp.sum(got_ref[...], axis=0)))
    tp_ref[...] = tp1_ref[...] - jnp.log(joined(own[...], g1[...], g2[...], g3[...]))


def call(kernel, shapes, args, scratch=(), specs=None, limit=24):
    return pl.pallas_call(
        kernel,
        out_shape=[jax.ShapeDtypeStruct(s, jnp.float32) for s in shapes],
        in_specs=specs or [VMEM] * len(args),
        out_specs=[VMEM] * len(shapes),
        scratch_shapes=list(scratch),
        compiler_params=pltpu.CompilerParams(vmem_limit_bytes=limit * 1024 * 1024),
    )(*args)


def over_tokens(array, axes):
    return lax.all_to_all(array, axes, split_axis=0, concat_axis=0, tiled=True)


def over_experts(array, axis):
    members = range(lax.axis_size(axis))
    return [array] + [
        lax.ppermute(array, axis, [(i, i ^ s) for i in members]) for s in members if s
    ]


def per_device(logits):
    experts, tokens = logits.shape
    token_axes, expert_axis = ("gx", "gz"), "gy"
    token_shards, expert_shards = lax.axis_size(token_axes), lax.axis_size(expert_axis)
    cap = float(tokens * token_shards) / float(experts * expert_shards)
    log_cap = float(np.log(np.float32(cap)))
    rows = tokens // LANES
    big, flat, wide, one = (experts, tokens), (rows, LANES), (rows * SUB, LANES), (1, experts)
    to_rows = (token_shards, 1, experts)

    x, msg = call(
        row_lse_kernel, [big, to_rows], [logits],
        [pltpu.SemaphoreType.DMA((experts // SUB,))], [HBM], 49,
    )
    got = over_tokens(msg, token_axes)
    e, top, msg, ep1 = call(
        functools.partial(column_lse_kernel, log_cap),
        [big, wide, flat, one], [got, x], [pltpu.VMEM(wide, jnp.float32)],
    )
    got = over_experts(msg, expert_axis)
    msg, f, tp1 = call(first_rows_kernel, [to_rows, wide, flat], [*got, top, e])
    for step in range(1, ITERS):
        row_parts = over_tokens(msg, token_axes)
        (msg,) = call(
            functools.partial(columns_kernel, cap),
            [flat], [row_parts, f, e], [pltpu.VMEM(wide, jnp.float32)],
        )
        got = over_experts(msg, expert_axis)
        if step < ITERS - 1:
            (msg,) = call(
                rows_kernel, [to_rows], [*got, f, e], [pltpu.VMEM(flat, jnp.float32)]
            )
    tp, ep = call(
        functools.partial(last_kernel, log_cap),
        [flat, one], [*got, tp1, row_parts, ep1],
    )
    return tp.reshape(tokens), ep.reshape(experts)


def solution(mesh):
    in_specs = (P("gy", ("gx", "gz")),)
    out_specs = (P(("gx", "gz")), P("gy"))
    return jax.shard_map(
        per_device, mesh=mesh, in_specs=in_specs, out_specs=out_specs, check_vma=False
    )
```

```python
import functools

import numpy as np

import jax
import jax.numpy as jnp
from jax import lax
from jax.experimental import pallas as pl
from jax.experimental.pallas import tpu as pltpu
from jax.sharding import PartitionSpec as P

ITERS = 3
HEAD = (5, 4)
LANES = 128
SUB = 8
UNROLL = 128
VMEM = pl.BlockSpec(memory_space=pltpu.VMEM)
HBM = pl.BlockSpec(memory_space=pltpu.HBM)


def tile(ref, j):
    block = ref[:, pl.ds(pl.multiple_of(j * LANES, LANES), LANES)]
    return block.reshape(-1, SUB, LANES)


def classes(j):
    return pl.ds(pl.multiple_of(j * SUB, SUB), SUB)


def class_rows(ref, block, s):
    return ref[pl.ds(block * SUB * SUB + s, SUB, stride=SUB), :]


def rows_to_lanes(values):
    return jnp.sum(values.T, axis=0, keepdims=True)


def lanes_to_rows(row):
    square = jnp.broadcast_to(row, (LANES, row.shape[1])).T
    return square.reshape(-1, SUB, LANES)


def for_tiles(count, body, carry):
    def step(k, carry):
        for n in range(UNROLL):
            carry = body(k * UNROLL + n, carry)
        return carry

    return lax.fori_loop(0, count // UNROLL, step, carry)


def row_lse_kernel(x_hbm, x_ref, msg_ref, sems):
    experts, tokens = x_ref.shape
    blocks = [pl.ds(g * SUB, SUB) for g in range(experts // SUB)]
    copies = [
        pltpu.make_async_copy(x_hbm.at[block, :], x_ref.at[block, :], sems.at[g])
        for g, block in enumerate(blocks)
    ]
    for copy in copies:
        copy.start()
    tops, totals = [], []
    for copy, block in zip(copies, blocks):
        copy.wait()
        starts = range(0, tokens, LANES)
        tree = [x_ref[block, pl.ds(s, LANES)] for s in starts]
        while len(tree) > 1:
            tree = [jnp.maximum(*pair) for pair in zip(tree[::2], tree[1::2])]
        top = tree[0]
        parts = [jnp.zeros((SUB, LANES), jnp.float32)] * 4
        for n, s in enumerate(starts):
            parts[n % 4] = parts[n % 4] + jnp.exp(x_ref[block, pl.ds(s, LANES)] - top)
        tops.append(top)
        totals.append((parts[0] + parts[1]) + (parts[2] + parts[3]))
    tops, totals = jnp.concatenate(tops).T, jnp.concatenate(totals).T
    peak = jnp.max(tops, axis=0, keepdims=True)
    summed = jnp.sum(totals * jnp.exp(tops - peak), axis=0, keepdims=True)
    msg_ref[...] = jnp.broadcast_to((peak + jnp.log(summed))[None], msg_ref.shape)


def column_lse_kernel(log_cap, got_ref, x_ref, e_ref, top_ref, msg_ref, ep_ref, sum_ref):
    tokens = x_ref.shape[1]
    parts = got_ref[...]
    most = jnp.max(parts, axis=0)
    ep = log_cap - (most + jnp.log(jnp.sum(jnp.exp(parts - most[None]), axis=0)))
    ep_ref[...] = ep
    shift = lanes_to_rows(ep)

    def body(j, carry):
        raised = tile(x_ref, j) + shift
        top = jnp.max(raised, axis=0)
        e = jnp.exp(raised - top[None])
        e_ref[:, pl.ds(pl.multiple_of(j * LANES, LANES), LANES)] = e.reshape(-1, LANES)
        top_ref[classes(j), :] = top
        sum_ref[classes(j), :] = jnp.sum(e, axis=0)
        return carry

    for_tiles(tokens // LANES, body, 0)
    for b in range(tokens // (LANES * SUB)):
        tops = [class_rows(top_ref, b, s) for s in range(SUB)]
        peak = functools.reduce(jnp.maximum, tops)
        total = sum(
            class_rows(sum_ref, b, s) * jnp.exp(tops[s] - peak) for s in range(SUB)
        )
        msg_ref[classes(b), :] = peak + jnp.log(total)


def joined(one, two, three, four):
    return (one + two) + (three + four)


def first_rows_kernel(own, g1, g2, g3, top_ref, e_ref, msg_ref, f_ref, tp_ref):
    experts, tokens = e_ref.shape
    parts = [ref[...] for ref in (own, g1, g2, g3)]
    peak = functools.reduce(jnp.maximum, parts)
    tp_ref[...] = -(peak + jnp.log(joined(*(jnp.exp(part - peak) for part in parts))))

    def body(j, acc):
        f = jnp.exp(top_ref[classes(j), :] + tp_ref[pl.ds(j, 1), :])
        f_ref[classes(j), :] = f
        return acc[1], acc[0] + tile(e_ref, j) * f[None]

    zero = jnp.zeros((experts // SUB, SUB, LANES), jnp.float32)
    acc = sum(for_tiles(tokens // LANES, body, (zero, zero)))
    msg_ref[...] = jnp.broadcast_to(
        rows_to_lanes(acc.reshape(experts, LANES))[None], msg_ref.shape
    )


def rows_kernel(own, g1, g2, g3, f_ref, e_ref, msg_ref, v_ref):
    experts, tokens = e_ref.shape
    v_ref[...] = 1.0 / joined(own[...], g1[...], g2[...], g3[...])

    def body(j, acc):
        w = f_ref[classes(j), :] * v_ref[pl.ds(j, 1), :]
        return acc[1], acc[0] + tile(e_ref, j) * w[None]

    zero = jnp.zeros((experts // SUB, SUB, LANES), jnp.float32)
    acc = sum(for_tiles(tokens // LANES, body, (zero, zero)))
    msg_ref[...] = jnp.broadcast_to(
        rows_to_lanes(acc.reshape(experts, LANES))[None], msg_ref.shape
    )


def columns_kernel(cap, got_ref, f_ref, e_ref, msg_ref, sum_ref):
    tokens = e_ref.shape[1]
    u = lanes_to_rows(cap / jnp.sum(got_ref[...], axis=0))

    def body(j, carry):
        sum_ref[classes(j), :] = jnp.sum(tile(e_ref, j) * u, axis=0) * f_ref[classes(j), :]
        return carry

    for_tiles(tokens // LANES, body, 0)
    for b in range(tokens // (LANES * SUB)):
        msg_ref[classes(b), :] = sum(class_rows(sum_ref, b, s) for s in range(SUB))


def last_kernel(log_cap, own, g1, g2, g3, tp1_ref, got_ref, ep1_ref, tp_ref, ep_ref):
    ep_ref[...] = ep1_ref[...] + (log_cap - jnp.log(jnp.sum(got_ref[...], axis=0)))
    tp_ref[...] = tp1_ref[...] - jnp.log(joined(own[...], g1[...], g2[...], g3[...]))


def call(kernel, shapes, args, scratch=(), specs=None, limit=24):
    return pl.pallas_call(
        kernel,
        out_shape=[jax.ShapeDtypeStruct(s, jnp.float32) for s in shapes],
        in_specs=specs or [VMEM] * len(args),
        out_specs=[VMEM] * len(shapes),
        scratch_shapes=list(scratch),
        compiler_params=pltpu.CompilerParams(vmem_limit_bytes=limit * 1024 * 1024),
    )(*args)


def over_tokens(array, axes):
    members = list(range(lax.axis_size(axes)))
    head = HEAD[0] * lax.axis_size(axes[1]) + HEAD[1]
    return lax.all_to_all(
        array, axes, split_axis=0, concat_axis=0, tiled=True,
        axis_index_groups=[members[head:] + members[:head]],
    )


def over_experts(array, axis):
    members = range(lax.axis_size(axis))
    return [array] + [
        lax.ppermute(array, axis, [(i, i ^ s) for i in members]) for s in members if s
    ]


def per_device(logits):
    experts, tokens = logits.shape
    token_axes, expert_axis = ("gx", "gz"), "gy"
    token_shards, expert_shards = lax.axis_size(token_axes), lax.axis_size(expert_axis)
    cap = float(tokens * token_shards) / float(experts * expert_shards)
    log_cap = float(np.log(np.float32(cap)))
    rows = tokens // LANES
    big, flat, wide, one = (experts, tokens), (rows, LANES), (rows * SUB, LANES), (1, experts)
    to_rows = (token_shards, 1, experts)

    x, msg = call(
        row_lse_kernel, [big, to_rows], [logits],
        [pltpu.SemaphoreType.DMA((experts // SUB,))], [HBM], 49,
    )
    got = over_tokens(msg, token_axes)
    e, top, msg, ep1 = call(
        functools.partial(column_lse_kernel, log_cap),
        [big, wide, flat, one], [got, x], [pltpu.VMEM(wide, jnp.float32)],
    )
    got = over_experts(msg, expert_axis)
    msg, f, tp1 = call(first_rows_kernel, [to_rows, wide, flat], [*got, top, e])
    for step in range(1, ITERS):
        row_parts = over_tokens(msg, token_axes)
        (msg,) = call(
            functools.partial(columns_kernel, cap),
            [flat], [row_parts, f, e], [pltpu.VMEM(wide, jnp.float32)],
        )
        got = over_experts(msg, expert_axis)
        if step < ITERS - 1:
            (msg,) = call(
                rows_kernel, [to_rows], [*got, f, e], [pltpu.VMEM(flat, jnp.float32)]
            )
    tp, ep = call(
        functools.partial(last_kernel, log_cap),
        [flat, one], [*got, tp1, row_parts, ep1],
    )
    return tp.reshape(tokens), ep.reshape(experts)


def solution(mesh):
    in_specs = (P("gy", ("gx", "gz")),)
    out_specs = (P(("gx", "gz")), P("gy"))
    return jax.shard_map(
        per_device, mesh=mesh, in_specs=in_specs, out_specs=out_specs, check_vma=False
    )
```

```python
import functools

import numpy as np

import jax
import jax.numpy as jnp
from jax import lax
from jax.experimental import pallas as pl
from jax.experimental.pallas import tpu as pltpu
from jax.sharding import PartitionSpec as P

ITERS = 3
HEAD = (5, 4)
LANES = 128
SUB = 8
SMALLEST = 2.0**-45
VMEM = pl.BlockSpec(memory_space=pltpu.VMEM)
HBM = pl.BlockSpec(memory_space=pltpu.HBM)


def tile(ref, j):
    block = ref[:, pl.ds(pl.multiple_of(j * LANES, LANES), LANES)]
    return block.reshape(-1, SUB, LANES)


def classes(j):
    return pl.ds(pl.multiple_of(j * SUB, SUB), SUB)


def class_rows(ref, block, s):
    return ref[pl.ds(block * SUB * SUB + s, SUB, stride=SUB), :]


def rows_to_lanes(values):
    return jnp.sum(values.T, axis=0, keepdims=True)


def lanes_to_rows(row):
    square = jnp.broadcast_to(row, (LANES, row.shape[1])).T
    return square.reshape(-1, SUB, LANES)


def row_lse_kernel(x_hbm, h_ref, top_ref, msg_ref, x_ref, sems):
    experts, tokens = h_ref.shape
    blocks = [pl.ds(g * SUB, SUB) for g in range(experts // SUB)]
    copies = [
        pltpu.make_async_copy(x_hbm.at[block, :], x_ref.at[block, :], sems.at[g])
        for g, block in enumerate(blocks)
    ]
    for copy in copies:
        copy.start()
    tops, totals = [], []
    for copy, block in zip(copies, blocks):
        copy.wait()
        starts = range(0, tokens, LANES)
        tree = [x_ref[block, pl.ds(s, LANES)] for s in starts]
        while len(tree) > 1:
            tree = [jnp.maximum(*pair) for pair in zip(tree[::2], tree[1::2])]
        top = tree[0]
        parts = [jnp.zeros((SUB, LANES), jnp.float32)] * 4
        for n, s in enumerate(starts):
            h = jnp.exp(x_ref[block, pl.ds(s, LANES)] - top)
            h_ref[block, pl.ds(s, LANES)] = h
            parts[n % 4] = parts[n % 4] + h
        tops.append(top)
        totals.append((parts[0] + parts[1]) + (parts[2] + parts[3]))
    top_ref[...] = jnp.concatenate(tops)
    tops, totals = jnp.concatenate(tops).T, jnp.concatenate(totals).T
    peak = jnp.max(tops, axis=0, keepdims=True)
    summed = jnp.sum(totals * jnp.exp(tops - peak), axis=0, keepdims=True)
    msg_ref[...] = jnp.broadcast_to((peak + jnp.log(summed))[None], msg_ref.shape)


def column_sums(e_ref, weight, sum_ref):
    tokens = e_ref.shape[1]
    for j in range(tokens // LANES):
        sum_ref[classes(j), :] = jnp.sum(tile(e_ref, j) * weight, axis=0)
    for b in range(tokens // (LANES * SUB)):
        yield b, sum(class_rows(sum_ref, b, s) for s in range(SUB))


def column_lse_kernel(
    log_cap, got_ref, top_ref, x_hbm, h_ref, e_ref, w_ref, peak_ref, msg_ref, ep_ref, sum_ref, sem
):
    del h_ref
    tokens = e_ref.shape[1]
    parts = got_ref[...]
    most = jnp.max(parts, axis=0)
    ep = log_cap - (most + jnp.log(jnp.sum(jnp.exp(parts - most[None]), axis=0)))
    ep_ref[...] = ep
    shift = lanes_to_rows(ep)
    weight = jnp.exp(top_ref[...].reshape(-1, SUB, LANES) + shift)
    w_ref[...] = weight.reshape(-1, LANES)
    peak_ref[...] = jnp.zeros_like(peak_ref)
    heaviest = jnp.max(jnp.max(weight, axis=0), axis=0, keepdims=True)
    bound = jnp.maximum(heaviest, 1.0) * SMALLEST
    short = jnp.zeros((SUB, LANES), jnp.float32)
    for b, total in column_sums(e_ref, weight, sum_ref):
        msg_ref[classes(b), :] = jnp.log(total)
        short = jnp.maximum(short, jnp.where(total >= bound, 0.0, 1.0))

    @pl.when(jnp.max(short) > 0.0)
    def _():
        copy = pltpu.make_async_copy(x_hbm, e_ref, sem)
        copy.start()
        copy.wait()
        w_ref[...] = jnp.ones_like(w_ref)

        def body(j, carry):
            raised = tile(e_ref, j) + shift
            peak = jnp.max(jnp.max(raised, axis=0), axis=0, keepdims=True)
            e = jnp.exp(raised - peak[None])
            e_ref[:, pl.ds(pl.multiple_of(j * LANES, LANES), LANES)] = e.reshape(-1, LANES)
            peak_ref[pl.ds(j, 1), :] = peak
            total = jnp.sum(jnp.sum(e, axis=0), axis=0, keepdims=True)
            msg_ref[pl.ds(j, 1), :] = peak + jnp.log(total)
            return carry

        lax.fori_loop(0, tokens // LANES, body, 0)


def joined(one, two, three, four):
    return (one + two) + (three + four)


def weighted_rows(e_ref, w_ref, v_ref, msg_ref):
    experts, tokens = e_ref.shape
    acc = [jnp.zeros((experts // SUB, SUB, LANES), jnp.float32)] * 2
    for j in range(tokens // LANES):
        acc[j % 2] = acc[j % 2] + tile(e_ref, j) * v_ref[pl.ds(j, 1), :][None]
    total = (acc[0] + acc[1]).reshape(experts, LANES) * w_ref[...]
    msg_ref[...] = jnp.broadcast_to(rows_to_lanes(total)[None], msg_ref.shape)


def first_rows_kernel(own, g1, g2, g3, peak_ref, w_ref, e_ref, msg_ref, f_ref, tp_ref):
    parts = [ref[...] for ref in (own, g1, g2, g3)]
    peak = functools.reduce(jnp.maximum, parts)
    tp = -(peak + jnp.log(joined(*(jnp.exp(part - peak) for part in parts))))
    tp_ref[...] = tp
    f_ref[...] = jnp.exp(peak_ref[...] + tp)
    weighted_rows(e_ref, w_ref, f_ref, msg_ref)


def rows_kernel(own, g1, g2, g3, f_ref, w_ref, e_ref, msg_ref, v_ref):
    v_ref[...] = f_ref[...] / joined(own[...], g1[...], g2[...], g3[...])
    weighted_rows(e_ref, w_ref, v_ref, msg_ref)


def columns_kernel(cap, got_ref, f_ref, w_ref, e_ref, msg_ref, sum_ref):
    u = lanes_to_rows(cap / jnp.sum(got_ref[...], axis=0))
    weight = u * w_ref[...].reshape(-1, SUB, LANES)
    for b, total in column_sums(e_ref, weight, sum_ref):
        msg_ref[classes(b), :] = f_ref[classes(b), :] * total


def last_kernel(log_cap, own, g1, g2, g3, tp1_ref, got_ref, ep1_ref, tp_ref, ep_ref):
    ep_ref[...] = ep1_ref[...] + (log_cap - jnp.log(jnp.sum(got_ref[...], axis=0)))
    tp_ref[...] = tp1_ref[...] - jnp.log(joined(own[...], g1[...], g2[...], g3[...]))


def call(kernel, shapes, args, scratch=(), specs=None, limit=24, aliases=None):
    return pl.pallas_call(
        kernel,
        out_shape=[jax.ShapeDtypeStruct(s, jnp.float32) for s in shapes],
        in_specs=specs or [VMEM] * len(args),
        out_specs=[VMEM] * len(shapes),
        scratch_shapes=list(scratch),
        input_output_aliases=aliases or {},
        compiler_params=pltpu.CompilerParams(vmem_limit_bytes=limit * 1024 * 1024),
    )(*args)


def over_tokens(array, axes):
    members = list(range(lax.axis_size(axes)))
    head = HEAD[0] * lax.axis_size(axes[1]) + HEAD[1]
    return lax.all_to_all(
        array, axes, split_axis=0, concat_axis=0, tiled=True,
        axis_index_groups=[members[head:] + members[:head]],
    )


def over_experts(array, axis):
    members = range(lax.axis_size(axis))
    return [array] + [
        lax.ppermute(array, axis, [(i, i ^ s) for i in members]) for s in members if s
    ]


def per_device(logits):
    experts, tokens = logits.shape
    token_axes, expert_axis = ("gx", "gz"), "gy"
    token_shards, expert_shards = lax.axis_size(token_axes), lax.axis_size(expert_axis)
    cap = float(tokens * token_shards) / float(experts * expert_shards)
    log_cap = float(np.log(np.float32(cap)))
    rows = tokens // LANES
    big, flat, wide, one = (experts, tokens), (rows, LANES), (rows * SUB, LANES), (1, experts)
    to_rows = (token_shards, 1, experts)

    lanes = (experts, LANES)
    h, top, msg = call(
        row_lse_kernel, [big, lanes, to_rows], [logits],
        [pltpu.VMEM(big, jnp.float32), pltpu.SemaphoreType.DMA((experts // SUB,))], [HBM], 49,
    )
    got = over_tokens(msg, token_axes)
    e, w, peak, msg, ep1 = call(
        functools.partial(column_lse_kernel, log_cap),
        [big, lanes, flat, flat, one], [got, top, logits, h],
        [pltpu.VMEM(wide, jnp.float32), pltpu.SemaphoreType.DMA],
        [VMEM, VMEM, HBM, VMEM], 49, {3: 0},
    )
    got = over_experts(msg, expert_axis)
    msg, f, tp1 = call(first_rows_kernel, [to_rows, flat, flat], [*got, peak, w, e])
    for step in range(1, ITERS):
        row_parts = over_tokens(msg, token_axes)
        (msg,) = call(
            functools.partial(columns_kernel, cap),
            [flat], [row_parts, f, w, e], [pltpu.VMEM(wide, jnp.float32)],
        )
        got = over_experts(msg, expert_axis)
        if step < ITERS - 1:
            (msg,) = call(
                rows_kernel, [to_rows], [*got, f, w, e], [pltpu.VMEM(flat, jnp.float32)]
            )
    tp, ep = call(
        functools.partial(last_kernel, log_cap),
        [flat, one], [*got, tp1, row_parts, ep1],
    )
    return tp.reshape(tokens), ep.reshape(experts)


def solution(mesh):
    in_specs = (P("gy", ("gx", "gz")),)
    out_specs = (P(("gx", "gz")), P("gy"))
    return jax.shard_map(
        per_device, mesh=mesh, in_specs=in_specs, out_specs=out_specs, check_vma=False
    )
```
